32 devices in a mesh: lat: 16 (over z, x, core), chan: 2 (over y).
Axes of the slice: x: 2, y: 2, z: 4, core: 2. Of those that a mesh axis runs over, the one named last changes fastest.
Arguments:
- spec_in: bfloat16 [384, 1, 256, 2, 384], P('lat', None, 'chan'), may hold values from -6 to 6
- legendre: float32 [384, 384, 384], P('lat'), may hold values from -0.4375 to 0.4375
- mode_slot: int32 [384], replicated, may hold values from 0 to 383, each once
- w_in: bfloat16 [512, 256], replicated, may hold values from -0.375 to 0.375
- b_in: float32 [512], replicated, may hold values from -3 to 3
- w_out: bfloat16 [256, 512], replicated, may hold values from -0.25 to 0.25
- kernel: float32 [256, 9], P('chan'), may hold values from -4 to 4
Outputs:
- spec_out: bfloat16 [384, 1, 256, 2, 384], P('lat', None, 'chan')
The draws below stay inside these ranges and needn't reach their ends.
Inputs may be any that keep to these rules, and one draw needn't show every extreme that they name: mode_slot holds every number of 0 to 383 once.
All inputs are finite; a program needn't handle non-finite values.
Results may differ from the reference program's by a relative error of at most 0.0083.
Values may be sent and summed in bfloat16 or wider, within the bound.
A program may use at most 192 MiB of HBM per device.

```python
import math
import jax
import jax.numpy as jnp
from jax import lax

C = 256
H = 512
NLAT = 384
NLON = 768
M = 384
L = 384
B = 1


def steps_of(rng, shape, pieces, low, high):
    gain, own = 1.0, jax.random.fold_in(rng, 6)
    for axis_at, parts in pieces:
        draws = jnp.exp(jax.random.uniform(jax.random.fold_in(own, axis_at), (parts,), jnp.float32, low / len(pieces), high / len(pieces)))
        gain = gain * jnp.repeat(draws, shape[axis_at] // parts).reshape([-1 if axis == axis_at else 1 for axis in range(len(shape))])
    return gain


def scatter_about(key, extent, deviation, most, pieces=(), kind=jnp.bfloat16):
    drawn = deviation * jax.random.normal(key, extent, jnp.float32)
    if pieces:
        drawn = drawn * steps_of(key, extent, pieces, -0.22, 0.18)
    return jnp.clip(drawn, -most, most).astype(kind)


def setup_inputs(seed: int = 0) -> dict:
    key_list = jax.random.split(jax.random.key(seed), 8)
    spec_in = scatter_about(key_list[0], (M, B, C, 2, L), 1.0, 6.0, ((0, 16), (2, 2)))
    legendre = scatter_about(key_list[1], (M, NLAT, L), (L // 2) ** -0.5, 0.4375, ((0, 16),), jnp.float32)
    mode_slot = jax.random.permutation(key_list[2], M).astype(jnp.int32)
    w_in = scatter_about(key_list[3], (H, C), C ** -0.5, 0.375)
    b_in = scatter_about(key_list[4], (H,), 0.5, 3.0, (), jnp.float32)
    w_out = scatter_about(key_list[5], (C, H), H ** -0.5, 0.25)
    kernel = scatter_about(key_list[6], (C, 9), 0.3, 4.0, ((0, 2),), jnp.float32)
    return {"spec_in": spec_in, "legendre": legendre, "mode_slot": mode_slot, "w_in": w_in, "b_in": b_in, "w_out": w_out, "kernel": kernel}


def wave_table(modes, count):
    columns = jnp.arange(count, dtype=jnp.int32)
    phase = (modes[:, None] * columns[None, :]) % count
    angle = phase.astype(jnp.float32) * (2.0 * math.pi / count)
    factor = count ** -0.5
    return jnp.stack([jnp.cos(angle) * factor, -jnp.sin(angle) * factor], axis=1)


def reference(spec_in, legendre, mode_slot, w_in, b_in, w_out, kernel):
    high = lax.Precision.HIGHEST
    degrees = jnp.arange(L, dtype=jnp.int32)
    masked = jnp.where(degrees[None, None, :] >= mode_slot[:, None, None], legendre, jnp.float32(0.0))
    waves = wave_table(mode_slot, NLON)
    half = NLON // 2

    def one_sample(coeffs):
        coeff = jnp.einsum('scrl,stl->scrt', coeffs.astype(jnp.float32), masked, precision=high)
        grid = jnp.einsum('scrt,srp->tcp', coeff, waves, precision=high).astype(jnp.bfloat16)
        pre = jnp.einsum('kc,tcp->tkp', w_in.astype(jnp.float32), grid.astype(jnp.float32), precision=high)
        hidden = jax.nn.gelu(pre + b_in[None, :, None], approximate=True).astype(jnp.bfloat16)
        branch = jnp.einsum('ck,tkp->tcp', w_out.astype(jnp.float32), hidden.astype(jnp.float32), precision=high)
        mixed = (grid.astype(jnp.float32) + branch).astype(jnp.bfloat16)
        wide = mixed.astype(jnp.float32)
        rows = jnp.concatenate([jnp.roll(wide[0:1], half, axis=2), wide, jnp.roll(wide[-1:], half, axis=2)], axis=0)
        conv = jnp.zeros_like(wide)
        for i in range(3):
            band = rows[i:i + NLAT]
            for j in range(3):
                conv = conv + kernel[:, 3 * i + j][None, :, None] * jnp.roll(band, 1 - j, axis=2)
        field = wide + conv
        modes = jnp.einsum('tcp,srp->scrt', field, waves, precision=high)
        return jnp.einsum('scrt,stl->scrl', modes, masked, precision=high).astype(jnp.bfloat16)

    result = lax.map(one_sample, jnp.moveaxis(spec_in, 1, 0))
    return jnp.moveaxis(result, 0, 1)
```

```python
import functools
import math

import jax
import jax.numpy as jnp
from jax import lax
from jax.experimental import pallas as pl
from jax.experimental.pallas import tpu as pltpu
from jax.sharding import PartitionSpec as P

NLON = 768


def with_halo(array, sides, width):
    for axis, dim in sides:
        count, length = (lax.axis_size(axis), array.shape[dim])
        up = [(i, (i + 1) % count) for i in range(count - 1)]
        down = [(j, i) for i, j in up]
        last = lax.slice_in_dim(array, length - width, length, axis=dim)
        first = lax.slice_in_dim(array, 0, width, axis=dim)
        before = lax.ppermute(last, axis, up)
        after = lax.ppermute(first, axis, down)
        array = jnp.concatenate([before, array, after], axis=dim)
    return array


def wave_table(modes, count):
    columns = jnp.arange(count, dtype=jnp.int32)
    phase = modes[:, None] * columns[None, :] % count
    angle = phase.astype(jnp.float32) * (2.0 * math.pi / count)
    factor = count ** (-0.5)
    return jnp.stack([jnp.cos(angle) * factor, -jnp.sin(angle) * factor], axis=1)


def on_device(spec_in, legendre, mode_slot, w_in, b_in, w_out, kernel):
    high = lax.Precision.HIGHEST
    slots_here = legendre.shape[0]
    lat_index = lax.axis_index("lat")
    local_modes = lax.dynamic_slice_in_dim(mode_slot, lat_index * slots_here, slots_here)
    degrees = jnp.arange(legendre.shape[2], dtype=jnp.int32)
    masked = jnp.where(
        degrees[None, None, :] >= local_modes[:, None, None], legendre, jnp.float32(0.0)
    )
    waves = wave_table(mode_slot, NLON)
    coeff = jnp.einsum("sbcrl,stl->sbcrt", spec_in.astype(jnp.float32), masked, precision=high)
    grid = jnp.einsum(
        "sbcrt,srp->btcp",
        lax.all_to_all(coeff, "lat", split_axis=4, concat_axis=0, tiled=True),
        waves,
        precision=high,
    ).astype(jnp.bfloat16)
    batch, rows_here, chan_here, columns = grid.shape
    whole = lax.all_gather(grid, "chan", axis=2, tiled=True)
    chan_index = lax.axis_index("chan")
    w_local = lax.dynamic_slice_in_dim(w_out, chan_index * chan_here, chan_here, 0)
    pre = jnp.einsum("hc,btcp->bthp", w_in, whole, preferred_element_type=jnp.float32)
    hidden = jax.nn.gelu(pre + b_in[None, None, :, None], approximate=True).astype(jnp.bfloat16)
    branch = jnp.einsum("ch,bthp->btcp", w_local, hidden, preferred_element_type=jnp.float32)
    mixed = (grid.astype(jnp.float32) + branch).astype(jnp.bfloat16)
    half = columns // 2
    last_row = lax.axis_size("lat") - 1
    padded = with_halo(mixed, (("lat", 1),), 1)
    upper = jnp.where(lat_index == 0, jnp.roll(mixed[:, 0:1], half, axis=3), padded[:, 0:1])
    lower = jnp.where(lat_index == last_row, jnp.roll(mixed[:, -1:], half, axis=3), padded[:, -1:])
    stacked = jnp.concatenate([upper, padded[:, 1:-1], lower], axis=1).astype(jnp.float32)
    wide = mixed.astype(jnp.float32)
    conv = jnp.zeros_like(wide)
    for i in range(3):
        band = stacked[:, i : i + rows_here]
        for j in range(3):
            conv = conv + kernel[:, 3 * i + j][None, None, :, None] * jnp.roll(band, 1 - j, axis=3)
    field = wide + conv
    modes = jnp.einsum("btcp,srp->sbcrt", field, waves, precision=high)
    return jnp.einsum(
        "sbcrt,stl->sbcrl",
        lax.all_to_all(modes, "lat", split_axis=0, concat_axis=4, tiled=True),
        masked,
        precision=high,
    ).astype(jnp.bfloat16)


def all_taps(taps, axis):
    count, index, width = lax.axis_size(axis), lax.axis_index(axis), taps.shape[1]
    ring = [(i, (i + 1) % count) for i in range(count)]
    whole = jnp.zeros((taps.shape[0], count * width), taps.dtype)
    for step in range(count):
        owner = (index - step) % count
        whole = lax.dynamic_update_slice_in_dim(whole, taps, owner * width, 1)
        if step < count - 1:
            taps = lax.ppermute(taps, axis, ring)
    return whole


def conv_halo(mixed, axes):
    count, index = lax.axis_size(axes), lax.axis_index(axes)
    half = mixed.shape[1] // 2
    up = [(i, i + 1) for i in range(count - 1)]
    down = [(j, i) for i, j in up]
    before = lax.ppermute(mixed[-1], axes, up)
    after = lax.ppermute(mixed[0], axes, down)
    before = jnp.where(index == 0, jnp.roll(mixed[0], half, axis=0), before)
    after = jnp.where(index == count - 1, jnp.roll(mixed[-1], half, axis=0), after)
    return before, after


def grid_kernel(lats, chans, coeff_ref, waves_ref, w_in_ref, b_in_ref, w_out_ref, mixed_ref):
    rows, width = coeff_ref.shape[2], coeff_ref.shape[3]
    coeff = coeff_ref[...].reshape(lats, chans, rows, width)
    parts = [coeff[:, j].reshape(lats * rows, width) for j in range(chans)]
    merged = jnp.concatenate(parts, axis=1)
    grid = jnp.dot(waves_ref[...], merged, preferred_element_type=jnp.float32).astype(jnp.bfloat16)
    pre = jnp.dot(grid, w_in_ref[...], preferred_element_type=jnp.float32) + b_in_ref[...]
    hidden = jax.nn.gelu(pre, approximate=True).astype(jnp.bfloat16)
    branch = jnp.dot(hidden, w_out_ref[...], preferred_element_type=jnp.float32)
    mixed_ref[0] = (grid.astype(jnp.float32) + branch).astype(jnp.bfloat16)


def field_kernel(lats, chans, here_ref, prev_ref, next_ref, before_ref, after_ref, kernel_ref, waves_ref, modes_ref):
    row, last = pl.program_id(0), pl.num_programs(0) - 1
    here = here_ref[0].astype(jnp.float32)
    prev = jnp.where(row == 0, before_ref[...].astype(jnp.float32), prev_ref[0].astype(jnp.float32))
    after = jnp.where(row == last, after_ref[...].astype(jnp.float32), next_ref[0].astype(jnp.float32))
    count = here.shape[0]
    taps = [
        kernel_ref[j : j + 1] * prev + kernel_ref[3 + j : 4 + j] * here + kernel_ref[6 + j : 7 + j] * after
        for j in range(3)
    ]
    field = here + taps[1] + pltpu.roll(taps[0], 1, 0) + pltpu.roll(taps[2], count - 1, 0)
    modes = jnp.dot(waves_ref[...], field.astype(jnp.bfloat16), preferred_element_type=jnp.float32)
    modes = modes.astype(jnp.bfloat16)
    rows, width = modes_ref.shape[2], modes_ref.shape[3]
    for i in range(lats):
        for j in range(chans):
            modes_ref[i * chans + j, 0] = modes[i * rows : (i + 1) * rows, j * width : (j + 1) * width]


def on_device_rows(spec_in, legendre, mode_slot, w_in, b_in, w_out, kernel):
    axes = ("lat", "chan")
    lats, chans = lax.axis_size("lat"), lax.axis_size("chan")
    count = lats * chans
    slots, rows_all, degrees_all = legendre.shape
    width = spec_in.shape[2]
    rows = rows_all // count
    columns = NLON
    channels = width * chans
    lat_index = lax.axis_index("lat")
    local_modes = lax.dynamic_slice_in_dim(mode_slot, lat_index * slots, slots)
    degrees = jnp.arange(degrees_all, dtype=jnp.int32)
    keep = degrees[None, None, :] >= local_modes[:, None, None]
    masked = jnp.where(keep, legendre, jnp.float32(0.0)).astype(jnp.bfloat16)
    waves = wave_table(mode_slot, columns).astype(jnp.bfloat16)
    waves = jnp.swapaxes(waves.reshape(lats, slots, 2, columns), 1, 2).reshape(-1, columns)
    taps = all_taps(kernel.T, "chan")
    coeff = jnp.einsum("scrl,stl->trsc", spec_in[:, 0], masked, preferred_element_type=jnp.float32)
    coeff = coeff.astype(jnp.bfloat16).reshape(rows_all, 2 * slots, width)
    coeff = lax.all_to_all(coeff, axes, split_axis=0, concat_axis=0, tiled=True)
    coeff = coeff.reshape(count, rows, 2 * slots, width)
    packed = pl.BlockSpec((count, 1, 2 * slots, width), lambda t: (0, t, 0, 0))

    def whole(array):
        return pl.BlockSpec(array.shape, lambda t: (0,) * array.ndim)

    w_in_t, w_out_t, bias, waves_t = w_in.T, w_out.T, b_in[None, :], waves.T
    params = pltpu.CompilerParams(vmem_limit_bytes=48 * 1024 * 1024)

    def mixed_rows(steps, stride, name):
        work = columns * channels * (waves_t.shape[1] + 2 * w_in_t.shape[1])
        return pl.pallas_call(
            functools.partial(grid_kernel, lats, chans),
            grid=(steps,),
            out_shape=jax.ShapeDtypeStruct((steps, columns, channels), jnp.bfloat16),
            in_specs=[
                pl.BlockSpec((count, 1, 2 * slots, width), lambda t: (0, t * stride, 0, 0)),
                whole(waves_t), whole(w_in_t), whole(bias), whole(w_out_t),
            ],
            out_specs=pl.BlockSpec((1, columns, channels), lambda t: (t, 0, 0)),
            compiler_params=params,
            cost_estimate=pl.CostEstimate(
                flops=2 * steps * work, bytes_accessed=coeff.nbytes, transcendentals=0
            ),
            name=name,
        )(coeff, waves_t, w_in_t, bias, w_out_t)

    edges = mixed_rows(min(2, rows), max(rows - 1, 1), "grid_edges")
    before, after = conv_halo(edges, axes)
    mixed = mixed_rows(rows, 1, "grid_mlp")
    line = (1, columns, channels)
    modes = pl.pallas_call(
        functools.partial(field_kernel, lats, chans),
        grid=(rows,),
        out_shape=jax.ShapeDtypeStruct((count, rows, 2 * slots, width), jnp.bfloat16),
        in_specs=[
            pl.BlockSpec(line, lambda t: (t, 0, 0)),
            pl.BlockSpec(line, lambda t: (jnp.maximum(t - 1, 0), 0, 0)),
            pl.BlockSpec(line, lambda t: (jnp.minimum(t + 1, rows - 1), 0, 0)),
            whole(before),
            whole(after),
            whole(taps),
            whole(waves),
        ],
        out_specs=packed,
        compiler_params=params,
        name="conv_dft",
    )(mixed, mixed, mixed, before, after, taps, waves)
    modes = modes.reshape(rows_all, 2 * slots, width)
    modes = lax.all_to_all(modes, axes, split_axis=0, concat_axis=0, tiled=True)
    modes = modes.reshape(rows_all, 2, slots, width)
    out = jnp.einsum("trsc,stl->scrl", modes, masked, preferred_element_type=jnp.float32)
    return out.astype(jnp.bfloat16)[:, None]


def solution(mesh):
    in_specs = (
        P("lat", None, "chan", None, None),
        P("lat", None, None),
        P(),
        P(),
        P(),
        P(),
        P("chan", None),
    )
    out_specs = P("lat", None, "chan", None, None)
    count = mesh.shape["lat"] * mesh.shape["chan"]

    def call(spec_in, legendre, *rest):
        samples, rows_all = spec_in.shape[1], legendre.shape[1]
        by_rows = samples == 1 and rows_all % count == 0
        body = on_device_rows if by_rows else on_device
        return jax.shard_map(
            body, mesh=mesh, in_specs=in_specs, out_specs=out_specs, check_vma=False
        )(spec_in, legendre, *rest)

    return call
```
